32 devices in a mesh: view: 4 (over x, core), gauss: 8 (over z, y).
Axes of the slice: x: 2, y: 2, z: 4, core: 2. Of those that a mesh axis runs over, the one named last changes fastest.
Arguments:
- means: float32 [3, 131072], P(None, 'gauss'), may hold values from -1 to 1
- scales: float32 [3, 131072], P(None, 'gauss'), may hold values from 0.05 to 0.6
- quats: float32 [4, 131072], P(None, 'gauss'), may hold values from -6 to 6
- attrs: float32 [49, 131072], P(None, 'gauss'), may hold values from -6 to 6
- grad_screen: float32 [16, 2, 131072], P('view', None, 'gauss'), may hold values from -6 to 6
- visible: int32 [16, 131072], P('view', 'gauss'), may hold values 0 or 1
- clone_mask: int32 [131072], P('gauss'), may hold values from 0 to 1, as said below
- rotation: float32 [16, 3, 3], P('view'), may hold values from -3.5 to 3.5
- shift: float32 [16, 3], P('view'), may hold values from 2 to 5
- focal: float32 [16], P('view'), may hold values from 1 to 4
Outputs:
- peak_stats: float32 [2, 131072], P(None, 'gauss')
- clones: float32 [61, 131072], P(None, 'gauss')
- clone_total: int32 [], replicated
The draws below stay inside these ranges and needn't reach their ends.
Inputs may be any that keep to these rules, and one draw needn't show every extreme that they name: `clone_mask`: in every draw some shard of 16384 consecutive Gaussians has all of them marked.
All inputs are finite; a program needn't handle non-finite values. No bound on the sum of `visible` on one device may be relied on, other than what follows from the above.
Results may differ from the reference program's by a relative error of at most 0.0003.
Values sent between devices are 32-bit elements; how exact they have to be, the bound alone decides.
A program may use at most 128 MiB of HBM per device.

```python
import math
import jax
import jax.numpy as jnp
from jax import lax

G_DEV = 16384
ATTR = 49
GAUSSIANS = 131072
VIEWS = 16
N_GAUSS = 8


def draw_clone_mask(key, part):
    shards = GAUSSIANS // G_DEV
    most = G_DEV // 128 * 128
    first, second, third = jax.random.split(key, 3)
    raw = jax.random.randint(first, (shards,), 0, most + 1)
    counts = raw * raw // most
    chosen = jax.random.randint(second, (), 0, shards)
    counts = jnp.where(jnp.arange(shards) == chosen, most, counts)
    keys = jax.random.split(third, shards)
    orders = jax.vmap(lambda k: jax.random.permutation(k, G_DEV))(keys)
    return (orders < counts[:, None]).astype(jnp.int32).reshape(-1)


def with_ends(result, stream_key, least, high):
    longest = result.shape.index(max(result.shape))
    spots = []
    for shift in (0, 1):
        where = [jax.random.randint(jax.random.fold_in(stream_key, axis), (), 0, length) for axis, length in enumerate(result.shape)]
        where[longest] = (where[longest] + shift) % result.shape[longest]
        spots.append(tuple(where))
    return result.at[spots[0]].set(least).at[spots[1]].set(high)


def level_of(own_key, extent, pieces, smallest, top_value):
    def one(dim, shards_of):
        steps = jax.random.uniform(jax.random.fold_in(jax.random.fold_in(own_key, 6), dim), (shards_of,), jnp.float32, smallest / len(pieces), top_value / len(pieces))
        return jnp.repeat(jnp.exp(steps), extent[dim] // shards_of).reshape((-1,) + (1,) * (len(extent) - dim - 1))

    loudness = one(*pieces[0])
    for cut in pieces[1:]:
        loudness = loudness * one(*cut)
    return loudness


def centred(own_key, dims, deviation, reach, cuts=(), dtype=jnp.bfloat16):
    result = deviation * jax.random.normal(own_key, dims, jnp.float32)
    if cuts:
        result = result * level_of(own_key, dims, cuts, -0.22, 0.18)
    return jnp.clip(result, -reach, reach).astype(dtype)


def setup_inputs(seed: int = 0) -> dict:
    arg_keys = jax.random.split(jax.random.key(seed), 11)
    return {
        "means": jnp.clip(jax.random.uniform(arg_keys[0], (3, GAUSSIANS), jnp.float32, -1.0, 1.0) * level_of(arg_keys[0], (3, GAUSSIANS), ((1, 8),), -0.4, 0.0), -1.0, 1.0),
        "scales": jnp.clip(jnp.exp(math.log(0.6) - 2.4849067 * jax.random.uniform(arg_keys[1], (3, GAUSSIANS), jnp.float32) ** level_of(arg_keys[1], (3, GAUSSIANS), ((1, 8),), -0.2, 0.2)), 0.05, 0.6),
        "quats": centred(arg_keys[2], (4, GAUSSIANS), 1.0, 6.0, ((1, 8),), jnp.float32),
        "attrs": centred(arg_keys[3], (ATTR, GAUSSIANS), 1.0, 6.0, ((1, 8),), jnp.float32),
        "grad_screen": centred(arg_keys[4], (VIEWS, 2, GAUSSIANS), 1.0, 6.0, ((0, 4), (2, 8)), jnp.float32),
        "visible": with_ends((jax.random.randint(arg_keys[5], (VIEWS, GAUSSIANS), 0, 4) < 3).astype(jnp.int32), jax.random.fold_in(arg_keys[5], 1), 0, 1),
        "clone_mask": draw_clone_mask(jax.random.fold_in(arg_keys[10], 71), 0),
        "rotation": centred(arg_keys[7], (VIEWS, 3, 3), 3 ** -0.5, 3.5, ((0, 4),), jnp.float32),
        "shift": jnp.clip(2.0 + 3.0 * jax.random.uniform(arg_keys[8], (VIEWS, 3), jnp.float32) ** level_of(arg_keys[8], (VIEWS, 3), ((0, 4),), -0.2, 0.2), 2.0, 5.0),
        "focal": jnp.clip(jnp.exp(math.log(4.0) - 1.3862944 * jax.random.uniform(arg_keys[9], (VIEWS,), jnp.float32) ** level_of(arg_keys[9], (VIEWS,), ((0, 4),), -0.2, 0.2)), 1.0, 4.0),
    }


def quat_factor(scales, quats):
    inv = 1.0 / jnp.sqrt(lax.optimization_barrier(jnp.sum(quats * quats, axis=0)) + 0.25)
    w, x, y, z = (quats[0] * inv, quats[1] * inv, quats[2] * inv, quats[3] * inv)
    rq = [[1 - 2 * (y * y + z * z), 2 * (x * y - w * z), 2 * (x * z + w * y)], [2 * (x * y + w * z), 1 - 2 * (x * x + z * z), 2 * (y * z - w * x)], [2 * (x * z - w * y), 2 * (y * z + w * x), 1 - 2 * (x * x + y * y)]]
    return [[rq[i][j] * scales[j] for j in range(3)] for i in range(3)]

def view_stats(means, factor, grad, seen, rot, trans, focal_v):
    point = [rot[i, 0] * means[0] + rot[i, 1] * means[1] + rot[i, 2] * means[2] + trans[i] for i in range(3)]
    depth = jnp.maximum(point[2], 1.0)
    j00 = focal_v / depth
    j02 = -focal_v * point[0] / (depth * depth)
    j12 = -focal_v * point[1] / (depth * depth)
    first = [j00 * rot[0, j] + j02 * rot[2, j] for j in range(3)]
    second = [j00 * rot[1, j] + j12 * rot[2, j] for j in range(3)]
    prow = [sum((first[j] * factor[j][k] for j in range(3))) for k in range(3)]
    qrow = [sum((second[j] * factor[j][k] for j in range(3))) for k in range(3)]
    a_val = prow[0] ** 2 + prow[1] ** 2 + prow[2] ** 2 + 0.3
    c_val = qrow[0] ** 2 + qrow[1] ** 2 + qrow[2] ** 2 + 0.3
    b_val = prow[0] * qrow[0] + prow[1] * qrow[1] + prow[2] * qrow[2]
    half = 0.5 * (a_val - c_val)
    lam = 0.5 * (a_val + c_val) + jnp.sqrt(half * half + b_val * b_val + 0.01)
    seenf = seen.astype(jnp.float32)
    radius = 3.0 * jnp.sqrt(lam) * seenf
    gnorm = jnp.sqrt(grad[0] * grad[0] + grad[1] * grad[1]) * seenf
    return (gnorm, radius)

def reference(means, scales, quats, attrs, grad_screen, visible, clone_mask, rotation, shift, focal):
    factor = quat_factor(scales, quats)
    gmax = jnp.zeros(means.shape[1], jnp.float32)
    rmax = jnp.zeros(means.shape[1], jnp.float32)
    for v in range(grad_screen.shape[0]):
        gnorm, radius = view_stats(means, factor, grad_screen[v], visible[v], rotation[v], shift[v], focal[v])
        gmax = jnp.maximum(gmax, gnorm)
        rmax = jnp.maximum(rmax, radius)
    peak = jnp.stack([gmax, rmax])
    rows = jnp.concatenate([means, scales, quats, attrs, peak], axis=0)
    shards = N_GAUSS
    cap = G_DEV // 128 * 128
    marks = clone_mask.reshape(shards, G_DEV)
    rank = jnp.cumsum(marks, axis=1).astype(jnp.int32) - 1
    counts = lax.optimization_barrier(jnp.sum(marks, axis=1)).astype(jnp.int32)
    blocks = (counts + 127) // 128
    offset = (jnp.cumsum(blocks) - blocks).astype(jnp.int32)
    block = offset[:, None] + rank // 128
    column = block % shards * cap + block // shards * 128 + rank % 128
    column = jnp.where(marks == 1, column, shards * cap).reshape(-1).astype(jnp.int32)
    clones = jnp.zeros((rows.shape[0], shards * cap), jnp.float32).at[:, column].set(rows, mode='drop')
    total = jnp.sum(clone_mask).astype(jnp.int32)
    return (peak, clones, total)
```

```python
import functools

import jax
import jax.numpy as jnp
from jax import lax
from jax.experimental import pallas as pl
from jax.experimental.pallas import tpu as pltpu
from jax.sharding import PartitionSpec as P

LANES = 128
SUB = 8
ATTR_TILES = 6
TILES = ATTR_TILES + 2
VMEM = pltpu.VMEM
SMEM = pltpu.SMEM
MESH = pl.DeviceIdType.MESH


def spec(space):
    return pl.BlockSpec(memory_space=space)


def peer(view, gauss):
    return {"view": view, "gauss": gauss}


def quat_factor(scales, quats):
    w, x, y, z = quats
    inv = 1.0 / jnp.sqrt(w * w + x * x + y * y + z * z + 0.25)
    w, x, y, z = (w * inv, x * inv, y * inv, z * inv)
    rq = [
        [1 - 2 * (y * y + z * z), 2 * (x * y - w * z), 2 * (x * z + w * y)],
        [2 * (x * y + w * z), 1 - 2 * (x * x + z * z), 2 * (y * z - w * x)],
        [2 * (x * z - w * y), 2 * (y * z + w * x), 1 - 2 * (x * x + y * y)],
    ]
    return [[rq[i][j] * scales[j] for j in range(3)] for i in range(3)]


def view_radius(means, factor, rot, trans, focal_v):
    point = [
        rot[i][0] * means[0] + rot[i][1] * means[1] + rot[i][2] * means[2] + trans[i]
        for i in range(3)
    ]
    inv = 1.0 / jnp.maximum(point[2], 1.0)
    j00 = focal_v * inv
    j02 = -(j00 * point[0]) * inv
    j12 = -(j00 * point[1]) * inv
    first = [j00 * rot[0][j] + j02 * rot[2][j] for j in range(3)]
    second = [j00 * rot[1][j] + j12 * rot[2][j] for j in range(3)]
    prow = [sum((first[j] * factor[j][k] for j in range(3))) for k in range(3)]
    qrow = [sum((second[j] * factor[j][k] for j in range(3))) for k in range(3)]
    a_val = prow[0] * prow[0] + prow[1] * prow[1] + prow[2] * prow[2] + 0.3
    c_val = qrow[0] * qrow[0] + qrow[1] * qrow[1] + qrow[2] * qrow[2] + 0.3
    b_val = prow[0] * qrow[0] + prow[1] * qrow[1] + prow[2] * qrow[2]
    half = 0.5 * (a_val - c_val)
    lam = 0.5 * (a_val + c_val) + jnp.sqrt(half * half + b_val * b_val + 0.01)
    return 3.0 * jnp.sqrt(lam)


def stats_kernel(
    V, S, views, par, mask, means, scales, quats, grad, vis, peak, meta,
    cnt, counts, local, halves, merged, whole,
    csend, crecv, rsend, rrecv, gsend, grecv,
):
    v, s = lax.axis_index("view"), lax.axis_index("gauss")
    nblk = mask.shape[0]
    piece = 2 * nblk // V
    cnt[...] = jnp.full((SUB, LANES), jnp.sum(mask[...]), jnp.int32)
    bar = pltpu.get_barrier_semaphore()
    for k in range(1, S):
        pl.semaphore_signal(bar, inc=1, device_id=peer(v, lax.rem(s + k, S)), device_id_type=MESH)
    for k in range(1, V):
        pl.semaphore_signal(bar, inc=1, device_id=peer(lax.rem(v + k, V), s), device_id_type=MESH)

    step = 2 * SUB

    def chunk(i, carry):
        rows = pl.ds(pl.multiple_of(i * step, step), step)
        m = [means[c, rows, :] for c in range(3)]
        factor = quat_factor(
            [scales[c, rows, :] for c in range(3)], [quats[c, rows, :] for c in range(4)]
        )
        gmax = jnp.zeros((step, LANES), jnp.float32)
        rmax = jnp.zeros((step, LANES), jnp.float32)
        for u in range(views):
            rot = [[par[u * 13 + 3 * a + b] for b in range(3)] for a in range(3)]
            trans = [par[u * 13 + 9 + a] for a in range(3)]
            radius = view_radius(m, factor, rot, trans, par[u * 13 + 12])
            seen = vis[u, rows, :].astype(jnp.float32)
            g0, g1 = grad[u, 0, rows, :], grad[u, 1, rows, :]
            gmax = jnp.maximum(gmax, jnp.sqrt(g0 * g0 + g1 * g1) * seen)
            rmax = jnp.maximum(rmax, radius * seen)
        local[rows, :] = gmax
        local[pl.ds(pl.multiple_of(nblk + i * step, step), step), :] = rmax
        return carry

    lax.fori_loop(0, nblk // step, chunk, 0)
    pl.semaphore_wait(bar, S + V - 2)
    copies = []
    for k in range(1, V):
        to = lax.rem(v + k, V)
        rs = pltpu.make_async_remote_copy(
            src_ref=local.at[pl.ds(pl.multiple_of(to * piece, piece), piece), :],
            dst_ref=halves.at[k],
            send_sem=rsend.at[k],
            recv_sem=rrecv.at[k],
            device_id=peer(to, s),
            device_id_type=MESH,
        )
        rs.start()
        copies.append(rs)
    tally = []
    for k in range(1, S):
        cp = pltpu.make_async_remote_copy(
            src_ref=cnt,
            dst_ref=counts.at[k],
            send_sem=csend.at[k],
            recv_sem=crecv.at[k],
            device_id=peer(v, lax.rem(s + k, S)),
            device_id_type=MESH,
        )
        cp.start()
        tally.append(cp)
    for rs in copies:
        rs.wait_recv()
    mine = pl.ds(pl.multiple_of(v * piece, piece), piece)
    best = local[mine, :]
    for k in range(1, V):
        best = jnp.maximum(best, halves[k])
    merged[...] = best
    spread = []
    for k in range(1, V):
        ag = pltpu.make_async_remote_copy(
            src_ref=merged,
            dst_ref=whole.at[k],
            send_sem=gsend.at[k],
            recv_sem=grecv.at[k],
            device_id=peer(lax.rem(v + k, V), s),
            device_id_type=MESH,
        )
        ag.start()
        spread.append(ag)
    for cp in tally:
        cp.wait_recv()
    lane = lax.broadcasted_iota(jnp.int32, (SUB, LANES), 1)
    sub = lax.broadcasted_iota(jnp.int32, (SUB, LANES), 0)
    blocks = jnp.zeros((SUB, LANES), jnp.int32)
    offs = jnp.zeros((SUB, LANES), jnp.int32)
    total = jnp.zeros((SUB, LANES), jnp.int32)
    for k in range(S):
        c = cnt[...] if k == 0 else counts[k]
        who = lax.rem(s + S - k, S)
        b = (c + (LANES - 1)) // LANES
        blocks = jnp.where(lane == who, b, blocks)
        offs = offs + jnp.where(lane > who, b, 0)
        total = total + c
    meta[...] = jnp.where(sub == 0, blocks, jnp.where(sub == 1, offs, total))
    peak[mine, :] = best
    for k in range(1, V):
        spread[k - 1].wait_recv()
        who = lax.rem(v + V - k, V)
        peak[pl.ds(pl.multiple_of(who * piece, piece), piece), :] = whole[k]
    for cp in copies + tally + spread:
        cp.wait_send()


def pack_kernel(
    V, S, T, per, meta, mask, attrs, last, means, scales, quats, peak, out,
    x, enc, basev, bases, sem, sem2,
):
    v, s = lax.axis_index("view"), lax.axis_index("gauss")
    nblk = mask.shape[0]
    for j in range(T):
        tile = v * T + j

        @pl.when(tile < ATTR_TILES)
        def _():
            pltpu.make_async_copy(
                attrs.at[pl.ds(pl.multiple_of(tile * SUB, SUB), SUB), :], x.at[j], sem.at[j]
            ).start()

    m = mask[...]
    lane = lax.broadcasted_iota(jnp.int32, (nblk, LANES), 1)
    mb = m.astype(jnp.bfloat16)
    li = lax.broadcasted_iota(jnp.int32, (LANES, LANES), 0)
    lj = lax.broadcasted_iota(jnp.int32, (LANES, LANES), 1)
    before = (li < lj).astype(jnp.bfloat16)
    bi = lax.broadcasted_iota(jnp.int32, (nblk, nblk), 0)
    bj = lax.broadcasted_iota(jnp.int32, (nblk, nblk), 1)
    above = (bi > bj).astype(jnp.bfloat16)
    under = (bi < bj).astype(jnp.bfloat16)
    dot = functools.partial(jnp.dot, preferred_element_type=jnp.float32)
    ones = jnp.ones((LANES, LANES), jnp.bfloat16)
    rank = dot(mb, before).astype(jnp.int32)
    size = dot(mb, ones).astype(jnp.int32)
    base = dot(dot(above, mb).astype(jnp.bfloat16), ones).astype(jnp.int32)
    flat = lax.dot_general(
        jnp.ones((SUB, LANES), jnp.bfloat16), mb, (((1,), (1,)), ((), ())),
        preferred_element_type=jnp.float32,
    )
    starts = dot(flat.astype(jnp.bfloat16), under)
    top = lax.broadcasted_iota(jnp.int32, (SUB, nblk), 0) == 0
    basev[...] = jnp.where(top, starts, starts + flat).astype(jnp.int32)
    scal = pltpu.make_async_copy(basev, bases, sem2)
    scal.start()
    code = jnp.where(m == 1, 65536 + (lane - rank) * 256 + lane, 0)
    bit = 1
    while bit < LANES:
        moved = pltpu.roll(code, LANES - bit, 1)
        goes = (moved & (bit * 256)) != 0
        stays = (code & (bit * 256)) == 0
        code = jnp.where(goes, moved, jnp.where(stays, code, 0))
        bit *= 2
    turn = (lane - base) & (LANES - 1)
    src = jnp.take_along_axis(code & (LANES - 1), turn, axis=1)
    enc[...] = jnp.where(turn < size, src, -1)

    for j in range(T):
        tile = v * T + j

        @pl.when(tile == ATTR_TILES)
        def _():
            x[j, 0:3, :] = means[...]
            x[j, 3:6, :] = scales[...]
            x[j, 6:8, :] = quats[0:2, :]

        @pl.when(tile == ATTR_TILES + 1)
        def _():
            x[j, 0:2, :] = quats[2:4, :]
            x[j, 2:3, :] = last[...]
            x[j, 3:5, :] = peak[...]
            x[j, 5:8, :] = jnp.zeros((3, peak.shape[1]), jnp.float32)

        @pl.when(tile < ATTR_TILES)
        def _():
            pltpu.make_async_copy(attrs.at[pl.ds(0, SUB), :], x.at[j], sem.at[j]).wait()

    out[...] = jnp.zeros_like(out)
    scal.wait()
    offset = meta[1, s]
    row = lax.broadcasted_iota(jnp.int32, (SUB, LANES), 1)

    def spot(d):
        return jnp.where(d < nblk, lax.rem(offset + d, S) * per + lax.div(d, S), S * per)

    def move(b, cur):
        start = bases[0, b]
        off = lax.rem(start, LANES)
        d = lax.div(start, LANES)
        e = jnp.broadcast_to(enc[pl.ds(b, 1), :], (SUB, LANES))
        idx = jnp.maximum(e, 0)
        ok = e >= 0
        low = ok & (row >= off)
        high = ok & (row < off)
        where = spot(d)
        cols = pl.ds(pl.multiple_of(b * LANES, LANES), LANES)
        full = bases[1, b] >= (d + 1) * LANES
        nxt = []
        for j in range(T):
            g = jnp.take_along_axis(x[j, :, cols], idx, axis=1)
            keep = jnp.where(low, g, cur[j])
            out[where, j * SUB:(j + 1) * SUB, :] = keep
            nxt.append(jnp.where(full, jnp.where(high, g, 0.0), keep))
        return tuple(nxt)

    zero = jnp.zeros((SUB, LANES), jnp.float32)
    cur = lax.fori_loop(0, nblk, move, (zero,) * T)
    end = lax.div(bases[1, nblk - 1], LANES)
    for j in range(T):
        out[spot(end), j * SUB:(j + 1) * SUB, :] = cur[j]


def ship_kernel(V, S, per, src, buf, gsend, vsend, csend, recv, lsem):
    v, s = lax.axis_index("view"), lax.axis_index("gauss")
    core = lax.rem(v, 2)
    mate = v + 1 - 2 * core
    X = V // 2
    bar = pltpu.get_barrier_semaphore()
    for k in range(1, S):
        pl.semaphore_signal(bar, inc=1, device_id=peer(v, lax.rem(s + k, S)), device_id_type=MESH)
    for q in range(1, X):
        pl.semaphore_signal(
            bar, inc=1, device_id=peer(lax.rem(v + 2 * q, V), s), device_id_type=MESH
        )
    pl.semaphore_signal(bar, inc=1, device_id=peer(mate, s), device_id_type=MESH)
    pl.semaphore_wait(bar, S - 1 + X)

    def part(i):
        return pl.ds(i * per, per)

    def far(k):
        to = lax.rem(s + k, S)
        return pltpu.make_async_remote_copy(
            src_ref=src.at[part(to)], dst_ref=buf.at[v, part(s)],
            send_sem=gsend.at[k], recv_sem=recv.at[0, k],
            device_id=peer(v, to), device_id_type=MESH,
        )

    def at(k, q):
        owner = lax.rem(v + V - 2 * q, V)
        frm = lax.rem(s + S - k, S)
        if k == 0 and q == 0:
            return src.at[part(s)], owner, frm
        return buf.at[owner, part(frm)], owner, frm

    def across(k, q):
        ref, _, frm = at(k, 0)
        return pltpu.make_async_remote_copy(
            src_ref=ref, dst_ref=buf.at[v, part(frm)],
            send_sem=vsend.at[q, k], recv_sem=recv.at[q, k],
            device_id=peer(lax.rem(v + 2 * q, V), s), device_id_type=MESH,
        )

    def beside(k, q):
        ref, owner, frm = at(k, q)
        return pltpu.make_async_remote_copy(
            src_ref=ref, dst_ref=buf.at[owner, part(frm)],
            send_sem=csend.at[q, k], recv_sem=recv.at[X + q, k],
            device_id=peer(mate, s), device_id_type=MESH,
        )

    started = []

    def go(copy):
        copy.start()
        started.append(copy)

    fars = {k: far(k) for k in range(1, S)}
    for k in range(1, S):
        go(fars[k])
    for q in range(1, X):
        go(across(0, q))
    go(beside(0, 0))
    own = pltpu.make_async_copy(src.at[part(s)], buf.at[v, part(s)], lsem)
    own.start()
    for k in range(S):
        if k:
            fars[k].wait_recv()
            for q in range(1, X):
                go(across(k, q))
            go(beside(k, 0))
        if k:
            for q in range(1, X):
                across(k - 1, q).wait_recv()
                go(beside(k - 1, q))
    for q in range(1, X):
        across(S - 1, q).wait_recv()
        go(beside(S - 1, q))
    for k in range(S):
        for q in range(X):
            beside(k, q).wait_recv()
    for copy in started:
        copy.wait_send()
    own.wait()


def place_kernel(S, T, per, meta, buf, out):
    me = lax.axis_index("gauss")
    slots = out.shape[1] // LANES
    sub = lax.broadcasted_iota(jnp.int32, (SUB, LANES), 0)
    rows = out.shape[0]
    head = sub < 2
    filled = jnp.int32(0)
    for s in range(S):
        blocks, offset = meta[0, s], meta[1, s]
        first = lax.rem(me + S - lax.rem(offset, S), S)
        n = lax.div(jnp.maximum(blocks - first, 0) + (S - 1), S)
        slot0 = lax.div(offset + first, S)

        def one(w, carry):
            t = []
            for tile in range(TILES):
                j = tile % T
                t.append(buf[tile // T, s * per + w, j * SUB:(j + 1) * SUB, :])
            turned = [pltpu.roll(a, 2, 0) for a in t[:ATTR_TILES]]
            mixed = t[ATTR_TILES + 1]
            chain = [mixed] + turned + [mixed]
            cols = pl.ds(pl.multiple_of((slot0 + w) * LANES, LANES), LANES)
            out[0:SUB, cols] = t[ATTR_TILES]
            for i in range(1, TILES):
                value = jnp.where(head, chain[i - 1], chain[i])
                hi = min((i + 1) * SUB, rows)
                out[i * SUB:hi, cols] = value[: hi - i * SUB]
            return carry

        lax.fori_loop(0, n, one, 0)
        filled = filled + n

    def clear(q, carry):
        cols = pl.ds(pl.multiple_of(q * LANES, LANES), LANES)
        out[:, cols] = jnp.zeros((rows, LANES), jnp.float32)
        return carry

    lax.fori_loop(filled, slots, clear, 0)


def body(V, S, means, scales, quats, attrs, grad_screen, visible, clone_mask, rotation, shift, focal):
    G = clone_mask.shape[0]
    nblk = G // LANES
    views = grad_screen.shape[0]
    rows = means.shape[0] + scales.shape[0] + quats.shape[0] + attrs.shape[0] + 2
    T = -(-TILES // V)
    per = -(-nblk // S)
    f32, i32 = jnp.float32, jnp.int32
    mask = clone_mask.reshape(nblk, LANES)
    par = jnp.concatenate(
        [rotation.reshape(views, 9), shift, focal[:, None]], axis=1
    ).reshape(-1)
    dma = pltpu.SemaphoreType.DMA
    piece = 2 * nblk // V
    peak2, meta = pl.pallas_call(
        functools.partial(stats_kernel, V, S, views),
        out_shape=(
            jax.ShapeDtypeStruct((2 * nblk, LANES), f32),
            jax.ShapeDtypeStruct((SUB, LANES), i32),
        ),
        in_specs=[spec(SMEM)] + [spec(VMEM)] * 6,
        out_specs=(spec(VMEM), spec(VMEM)),
        scratch_shapes=[
            VMEM((SUB, LANES), i32),
            VMEM((S, SUB, LANES), i32),
            VMEM((2 * nblk, LANES), f32),
            VMEM((V, piece, LANES), f32),
            VMEM((piece, LANES), f32),
            VMEM((V, piece, LANES), f32),
            dma((S,)), dma((S,)), dma((V,)), dma((V,)), dma((V,)), dma((V,)),
        ],
        compiler_params=pltpu.CompilerParams(collective_id=0, has_side_effects=True),
        name="stats",
    )(
        par, mask,
        means.reshape(3, nblk, LANES), scales.reshape(3, nblk, LANES),
        quats.reshape(4, nblk, LANES), grad_screen.reshape(views, 2, nblk, LANES),
        visible.reshape(views, nblk, LANES),
    )
    peak = peak2.reshape(2, G)
    total = meta[2, 0]
    R = T * SUB
    packed = pl.pallas_call(
        functools.partial(pack_kernel, V, S, T, per),
        out_shape=jax.ShapeDtypeStruct((S * per + 1, R, LANES), f32),
        in_specs=[spec(SMEM), spec(VMEM), spec(pl.ANY)] + [spec(VMEM)] * 5,
        out_specs=spec(VMEM),
        scratch_shapes=[
            VMEM((T, SUB, G), f32),
            VMEM((nblk, LANES), i32),
            VMEM((SUB, nblk), i32),
            SMEM((SUB, nblk), i32),
            dma((T,)), dma,
        ],
        name="pack",
    )(meta, mask, attrs, attrs[ATTR_TILES * SUB:], means, scales, quats, peak)
    X = V // 2
    buf = pl.pallas_call(
        functools.partial(ship_kernel, V, S, per),
        out_shape=jax.ShapeDtypeStruct((V, S * per, R, LANES), f32),
        in_specs=[spec(VMEM)],
        out_specs=spec(pl.ANY),
        scratch_shapes=[
            dma((S,)), dma((X, S)), dma((X, S)), dma((2 * X, S)), dma,
        ],
        compiler_params=pltpu.CompilerParams(collective_id=1, has_side_effects=True),
        name="ship",
    )(packed)
    clones = pl.pallas_call(
        functools.partial(place_kernel, S, T, per),
        out_shape=jax.ShapeDtypeStruct((rows, G), f32),
        in_specs=[spec(SMEM), spec(VMEM)],
        out_specs=spec(VMEM),
        compiler_params=pltpu.CompilerParams(vmem_limit_bytes=32 * 1024 * 1024),
        name="place",
    )(meta, buf)
    return peak, clones, total


def solution(mesh):
    return jax.shard_map(
        functools.partial(body, mesh.shape["view"], mesh.shape["gauss"]),
        mesh=mesh,
        in_specs=(
            P(None, "gauss"),
            P(None, "gauss"),
            P(None, "gauss"),
            P(None, "gauss"),
            P("view", None, "gauss"),
            P("view", "gauss"),
            P("gauss"),
            P("view", None, None),
            P("view", None),
            P("view"),
        ),
        out_specs=(P(None, "gauss"), P(None, "gauss"), P()),
        check_vma=False,
    )
```

```python
import functools

import jax
import jax.numpy as jnp
from jax import lax
from jax.experimental import pallas as pl
from jax.experimental.pallas import tpu as pltpu
from jax.sharding import PartitionSpec as P

LANES = 128
SUB = 8
ATTR_TILES = 6
TILES = ATTR_TILES + 2
VMEM = pltpu.VMEM
SMEM = pltpu.SMEM
MESH = pl.DeviceIdType.MESH


def spec(space):
    return pl.BlockSpec(memory_space=space)


def peer(view, gauss):
    return {"view": view, "gauss": gauss}


def quat_factor(scales, quats):
    w, x, y, z = quats
    inv = 1.0 / jnp.sqrt(w * w + x * x + y * y + z * z + 0.25)
    w, x, y, z = (w * inv, x * inv, y * inv, z * inv)
    rq = [
        [1 - 2 * (y * y + z * z), 2 * (x * y - w * z), 2 * (x * z + w * y)],
        [2 * (x * y + w * z), 1 - 2 * (x * x + z * z), 2 * (y * z - w * x)],
        [2 * (x * z - w * y), 2 * (y * z + w * x), 1 - 2 * (x * x + y * y)],
    ]
    return [[rq[i][j] * scales[j] for j in range(3)] for i in range(3)]


def view_radius(means, factor, rot, trans, focal_v):
    point = [
        rot[i][0] * means[0] + rot[i][1] * means[1] + rot[i][2] * means[2] + trans[i]
        for i in range(3)
    ]
    inv = 1.0 / jnp.maximum(point[2], 1.0)
    j00 = focal_v * inv
    j02 = -(j00 * point[0]) * inv
    j12 = -(j00 * point[1]) * inv
    first = [j00 * rot[0][j] + j02 * rot[2][j] for j in range(3)]
    second = [j00 * rot[1][j] + j12 * rot[2][j] for j in range(3)]
    prow = [sum((first[j] * factor[j][k] for j in range(3))) for k in range(3)]
    qrow = [sum((second[j] * factor[j][k] for j in range(3))) for k in range(3)]
    a_val = prow[0] * prow[0] + prow[1] * prow[1] + prow[2] * prow[2] + 0.3
    c_val = qrow[0] * qrow[0] + qrow[1] * qrow[1] + qrow[2] * qrow[2] + 0.3
    b_val = prow[0] * qrow[0] + prow[1] * qrow[1] + prow[2] * qrow[2]
    half = 0.5 * (a_val - c_val)
    lam = 0.5 * (a_val + c_val) + jnp.sqrt(half * half + b_val * b_val + 0.01)
    return 3.0 * jnp.sqrt(lam)


def stats_kernel(
    V, S, views, rots, trns, foc, mask, means, scales, quats, grad, vis, peak, meta,
    cnt, counts, local, halves, merged, whole, total_max,
    csend, crecv, rsend, rrecv, gsend, grecv,
):
    v, s = lax.axis_index("view"), lax.axis_index("gauss")
    nblk = mask.shape[0]
    piece = 2 * nblk // V
    cnt[...] = jnp.full((SUB, LANES), jnp.sum(mask[...]), jnp.int32)
    bar = pltpu.get_barrier_semaphore()
    for k in range(1, S):
        pl.semaphore_signal(bar, inc=1, device_id=peer(v, lax.rem(s + k, S)), device_id_type=MESH)
    for k in range(1, V):
        pl.semaphore_signal(bar, inc=1, device_id=peer(lax.rem(v + k, V), s), device_id_type=MESH)

    step = 2 * SUB

    def chunk(i, carry):
        rows = pl.ds(pl.multiple_of(i * step, step), step)

        def lines(ref, count, c):
            return ref[pl.ds(i * step * count + c, step, stride=count), :]

        m = [means[rows, c, :] for c in range(3)]
        factor = quat_factor(
            [scales[rows, c, :] for c in range(3)], [lines(quats, 4, c) for c in range(4)]
        )
        gmax = jnp.zeros((step, LANES), jnp.float32)
        rmax = jnp.zeros((step, LANES), jnp.float32)
        for u in range(views):
            rot = [[rots[u, a, b] for b in range(3)] for a in range(3)]
            trans = [trns[u, a] for a in range(3)]
            radius = view_radius(m, factor, rot, trans, foc[u])
            seen = lines(vis, views, u).astype(jnp.float32)
            g0, g1 = (grad[u, pl.ds(i * step * 2 + c, step, stride=2), :] for c in range(2))
            gmax = jnp.maximum(gmax, jnp.sqrt(g0 * g0 + g1 * g1) * seen)
            rmax = jnp.maximum(rmax, radius * seen)
        local[pl.ds(i * step * 2, step, stride=2), :] = gmax
        local[pl.ds(i * step * 2 + 1, step, stride=2), :] = rmax
        return carry

    lax.fori_loop(0, nblk // step, chunk, 0)
    pl.semaphore_wait(bar, S + V - 2)
    copies = []
    for k in range(1, V):
        to = lax.rem(v + k, V)
        rs = pltpu.make_async_remote_copy(
            src_ref=local.at[pl.ds(pl.multiple_of(to * piece, piece), piece), :],
            dst_ref=halves.at[k],
            send_sem=rsend.at[k],
            recv_sem=rrecv.at[k],
            device_id=peer(to, s),
            device_id_type=MESH,
        )
        rs.start()
        copies.append(rs)
    tally = []
    for k in range(1, S):
        cp = pltpu.make_async_remote_copy(
            src_ref=cnt,
            dst_ref=counts.at[k],
            send_sem=csend.at[k],
            recv_sem=crecv.at[k],
            device_id=peer(v, lax.rem(s + k, S)),
            device_id_type=MESH,
        )
        cp.start()
        tally.append(cp)
    for rs in copies:
        rs.wait_recv()
    mine = pl.ds(pl.multiple_of(v * piece, piece), piece)
    best = local[mine, :]
    for k in range(1, V):
        best = jnp.maximum(best, halves[k])
    merged[...] = best
    spread = []
    for k in range(1, V):
        ag = pltpu.make_async_remote_copy(
            src_ref=merged,
            dst_ref=whole.at[k],
            send_sem=gsend.at[k],
            recv_sem=grecv.at[k],
            device_id=peer(lax.rem(v + k, V), s),
            device_id_type=MESH,
        )
        ag.start()
        spread.append(ag)
    for cp in tally:
        cp.wait_recv()
    lane = lax.broadcasted_iota(jnp.int32, (SUB, LANES), 1)
    sub = lax.broadcasted_iota(jnp.int32, (SUB, LANES), 0)
    blocks = jnp.zeros((SUB, LANES), jnp.int32)
    offs = jnp.zeros((SUB, LANES), jnp.int32)
    total = jnp.zeros((SUB, LANES), jnp.int32)
    for k in range(S):
        c = cnt[...] if k == 0 else counts[k]
        who = lax.rem(s + S - k, S)
        b = (c + (LANES - 1)) // LANES
        blocks = jnp.where(lane == who, b, blocks)
        offs = offs + jnp.where(lane > who, b, 0)
        total = total + c
    meta[...] = jnp.where(sub == 0, blocks, jnp.where(sub == 1, offs, total))
    total_max[mine, :] = best
    for k in range(1, V):
        spread[k - 1].wait_recv()
        who = lax.rem(v + V - k, V)
        total_max[pl.ds(pl.multiple_of(who * piece, piece), piece), :] = whole[k]
    for c in range(2):
        peak[:, c, :] = total_max[pl.ds(c, nblk, stride=2), :]
    for cp in copies + tally + spread:
        cp.wait_send()


def pack_kernel(
    V, S, T, per, meta, mask, attrs, means, scales, quats, peak, out,
    x, enc, basev, bases, sem, sem2,
):
    v, s = lax.axis_index("view"), lax.axis_index("gauss")
    nblk = mask.shape[0]
    for j in range(T):
        tile = v * T + j

        @pl.when(tile < ATTR_TILES)
        def _():
            pltpu.make_async_copy(
                attrs.at[pl.ds(pl.multiple_of(tile * SUB, SUB), SUB), :], x.at[j], sem.at[j]
            ).start()

        @pl.when(tile == ATTR_TILES + 1)
        def _():
            pltpu.make_async_copy(
                attrs.at[pl.ds(ATTR_TILES * SUB, 1), :], x.at[j, pl.ds(2, 1), :], sem.at[j]
            ).start()

    m = mask[...]
    lane = lax.broadcasted_iota(jnp.int32, (nblk, LANES), 1)
    mb = m.astype(jnp.bfloat16)
    li = lax.broadcasted_iota(jnp.int32, (LANES, LANES), 0)
    lj = lax.broadcasted_iota(jnp.int32, (LANES, LANES), 1)
    before = (li < lj).astype(jnp.bfloat16)
    bi = lax.broadcasted_iota(jnp.int32, (nblk, nblk), 0)
    bj = lax.broadcasted_iota(jnp.int32, (nblk, nblk), 1)
    above = (bi > bj).astype(jnp.bfloat16)
    under = (bi < bj).astype(jnp.bfloat16)
    dot = functools.partial(jnp.dot, preferred_element_type=jnp.float32)
    ones = jnp.ones((LANES, LANES), jnp.bfloat16)
    rank = dot(mb, before).astype(jnp.int32)
    size = dot(mb, ones).astype(jnp.int32)
    base = dot(dot(above, mb).astype(jnp.bfloat16), ones).astype(jnp.int32)
    flat = lax.dot_general(
        jnp.ones((SUB, LANES), jnp.bfloat16), mb, (((1,), (1,)), ((), ())),
        preferred_element_type=jnp.float32,
    )
    starts = dot(flat.astype(jnp.bfloat16), under)
    top = lax.broadcasted_iota(jnp.int32, (SUB, nblk), 0) == 0
    basev[...] = jnp.where(top, starts, starts + flat).astype(jnp.int32)
    scal = pltpu.make_async_copy(basev, bases, sem2)
    scal.start()
    code = jnp.where(m == 1, 65536 + (lane - rank) * 256 + lane, 0)
    bit = 1
    while bit < LANES:
        moved = pltpu.roll(code, LANES - bit, 1)
        goes = (moved & (bit * 256)) != 0
        stays = (code & (bit * 256)) == 0
        code = jnp.where(goes, moved, jnp.where(stays, code, 0))
        bit *= 2
    turn = (lane - base) & (LANES - 1)
    src = jnp.take_along_axis(code & (LANES - 1), turn, axis=1)
    enc[...] = jnp.where(turn < size, src, -1)

    for j in range(T):
        tile = v * T + j

        @pl.when(tile == ATTR_TILES)
        def _():
            x[j, 0:3, :] = means[...]
            x[j, 3:6, :] = scales[...]
            x[j, 6:8, :] = quats[0:2, :]

        @pl.when(tile == ATTR_TILES + 1)
        def _():
            x[j, 0:2, :] = quats[2:4, :]
            x[j, 3:5, :] = peak[...]
            x[j, 5:8, :] = jnp.zeros((3, peak.shape[1]), jnp.float32)
            pltpu.make_async_copy(
                attrs.at[pl.ds(ATTR_TILES * SUB, 1), :], x.at[j, pl.ds(2, 1), :], sem.at[j]
            ).wait()

        @pl.when(tile < ATTR_TILES)
        def _():
            pltpu.make_async_copy(attrs.at[pl.ds(0, SUB), :], x.at[j], sem.at[j]).wait()

    out[...] = jnp.zeros_like(out)
    scal.wait()
    offset = meta[1, s]
    row = lax.broadcasted_iota(jnp.int32, (SUB, LANES), 1)

    def spot(d):
        return jnp.where(d < nblk, lax.rem(offset + d, S) * per + lax.div(d, S), S * per)

    def move(b, cur):
        start = bases[0, b]
        off = lax.rem(start, LANES)
        d = lax.div(start, LANES)
        e = jnp.broadcast_to(enc[pl.ds(b, 1), :], (SUB, LANES))
        idx = jnp.maximum(e, 0)
        ok = e >= 0
        low = ok & (row >= off)
        high = ok & (row < off)
        where = spot(d)
        cols = pl.ds(pl.multiple_of(b * LANES, LANES), LANES)
        full = bases[1, b] >= (d + 1) * LANES
        nxt = []
        for j in range(T):
            g = jnp.take_along_axis(x[j, :, cols], idx, axis=1)
            keep = jnp.where(low, g, cur[j])
            out[where, j * SUB:(j + 1) * SUB, :] = keep
            nxt.append(jnp.where(full, jnp.where(high, g, 0.0), keep))
        return tuple(nxt)

    zero = jnp.zeros((SUB, LANES), jnp.float32)
    cur = lax.fori_loop(0, nblk, move, (zero,) * T, unroll=8)
    end = lax.div(bases[1, nblk - 1], LANES)
    for j in range(T):
        out[spot(end), j * SUB:(j + 1) * SUB, :] = cur[j]


def ship_kernel(V, S, per, src, buf, gsend, vsend, csend, recv, lsem):
    v, s = lax.axis_index("view"), lax.axis_index("gauss")
    core = lax.rem(v, 2)
    mate = v + 1 - 2 * core
    X = V // 2
    bar = pltpu.get_barrier_semaphore()
    for k in range(1, S):
        pl.semaphore_signal(bar, inc=1, device_id=peer(v, lax.rem(s + k, S)), device_id_type=MESH)
    for q in range(1, X):
        pl.semaphore_signal(
            bar, inc=1, device_id=peer(lax.rem(v + 2 * q, V), s), device_id_type=MESH
        )
    pl.semaphore_signal(bar, inc=1, device_id=peer(mate, s), device_id_type=MESH)
    pl.semaphore_wait(bar, S - 1 + X)

    def part(i):
        return pl.ds(i * per, per)

    def far(k):
        to = lax.rem(s + k, S)
        return pltpu.make_async_remote_copy(
            src_ref=src.at[part(to)], dst_ref=buf.at[v, part(s)],
            send_sem=gsend.at[k], recv_sem=recv.at[0, k],
            device_id=peer(v, to), device_id_type=MESH,
        )

    def at(k, q):
        owner = lax.rem(v + V - 2 * q, V)
        frm = lax.rem(s + S - k, S)
        if k == 0 and q == 0:
            return src.at[part(s)], owner, frm
        return buf.at[owner, part(frm)], owner, frm

    def across(k, q):
        ref, _, frm = at(k, 0)
        return pltpu.make_async_remote_copy(
            src_ref=ref, dst_ref=buf.at[v, part(frm)],
            send_sem=vsend.at[q, k], recv_sem=recv.at[q, k],
            device_id=peer(lax.rem(v + 2 * q, V), s), device_id_type=MESH,
        )

    def beside(k, q):
        ref, owner, frm = at(k, q)
        return pltpu.make_async_remote_copy(
            src_ref=ref, dst_ref=buf.at[owner, part(frm)],
            send_sem=csend.at[q, k], recv_sem=recv.at[X + q, k],
            device_id=peer(mate, s), device_id_type=MESH,
        )

    started = []

    def go(copy):
        copy.start()
        started.append(copy)

    fars = {k: far(k) for k in range(1, S)}
    for k in range(1, S):
        go(fars[k])
    for q in range(1, X):
        go(across(0, q))
    go(beside(0, 0))
    own = pltpu.make_async_copy(src.at[part(s)], buf.at[v, part(s)], lsem)
    own.start()
    for k in range(S):
        if k:
            fars[k].wait_recv()
            for q in range(1, X):
                go(across(k, q))
            go(beside(k, 0))
        if k:
            for q in range(1, X):
                across(k - 1, q).wait_recv()
                go(beside(k - 1, q))
    for q in range(1, X):
        across(S - 1, q).wait_recv()
        go(beside(S - 1, q))
    for k in range(S):
        for q in range(X):
            beside(k, q).wait_recv()
    for copy in started:
        copy.wait_send()
    own.wait()


def place_kernel(S, T, per, meta, buf, out):
    me = lax.axis_index("gauss")
    slots = out.shape[1] // LANES
    sub = lax.broadcasted_iota(jnp.int32, (SUB, LANES), 0)
    rows = out.shape[0]
    head = sub < 2
    filled = jnp.int32(0)
    for s in range(S):
        blocks, offset = meta[0, s], meta[1, s]
        first = lax.rem(me + S - lax.rem(offset, S), S)
        n = lax.div(jnp.maximum(blocks - first, 0) + (S - 1), S)
        slot0 = lax.div(offset + first, S)

        def one(w, carry):
            t = []
            for tile in range(TILES):
                j = tile % T
                t.append(buf[tile // T, s * per + w, j * SUB:(j + 1) * SUB, :])
            turned = [pltpu.roll(a, 2, 0) for a in t[:ATTR_TILES]]
            mixed = t[ATTR_TILES + 1]
            chain = [mixed] + turned + [mixed]
            cols = pl.ds(pl.multiple_of((slot0 + w) * LANES, LANES), LANES)
            out[0:SUB, cols] = t[ATTR_TILES]
            for i in range(1, TILES):
                value = jnp.where(head, chain[i - 1], chain[i])
                hi = min((i + 1) * SUB, rows)
                out[i * SUB:hi, cols] = value[: hi - i * SUB]
            return carry

        lax.fori_loop(0, n, one, 0)
        filled = filled + n

    def clear(q, carry):
        cols = pl.ds(pl.multiple_of(q * LANES, LANES), LANES)
        out[:, cols] = jnp.zeros((rows, LANES), jnp.float32)
        return carry

    lax.fori_loop(filled, slots, clear, 0)


def body(V, S, means, scales, quats, attrs, grad_screen, visible, clone_mask, rotation, shift, focal):
    G = clone_mask.shape[0]
    nblk = G // LANES
    views = grad_screen.shape[0]
    rows = means.shape[0] + scales.shape[0] + quats.shape[0] + attrs.shape[0] + 2
    T = -(-TILES // V)
    per = -(-nblk // S)
    f32, i32 = jnp.float32, jnp.int32
    mask = clone_mask.reshape(nblk, LANES)

    def lines(a):
        a = a.reshape(a.shape[:-1] + (nblk, LANES))
        return jnp.swapaxes(a, -3, -2)

    dma = pltpu.SemaphoreType.DMA
    piece = 2 * nblk // V
    peak2, meta = pl.pallas_call(
        functools.partial(stats_kernel, V, S, views),
        out_shape=(
            jax.ShapeDtypeStruct((nblk, 2, LANES), f32),
            jax.ShapeDtypeStruct((SUB, LANES), i32),
        ),
        in_specs=[spec(SMEM)] * 3 + [spec(VMEM)] * 6,
        out_specs=(spec(VMEM), spec(VMEM)),
        scratch_shapes=[
            VMEM((SUB, LANES), i32),
            VMEM((S, SUB, LANES), i32),
            VMEM((2 * nblk, LANES), f32),
            VMEM((V, piece, LANES), f32),
            VMEM((piece, LANES), f32),
            VMEM((V, piece, LANES), f32),
            VMEM((2 * nblk, LANES), f32),
            dma((S,)), dma((S,)), dma((V,)), dma((V,)), dma((V,)), dma((V,)),
        ],
        compiler_params=pltpu.CompilerParams(collective_id=0, has_side_effects=True),
        name="stats",
    )(
        rotation, shift, focal, mask, lines(means), lines(scales),
        lines(quats).reshape(-1, LANES), lines(grad_screen).reshape(views, -1, LANES),
        lines(visible).reshape(-1, LANES),
    )
    peak = jnp.swapaxes(peak2, 0, 1).reshape(2, G)
    total = meta[2, 0]
    R = T * SUB
    packed = pl.pallas_call(
        functools.partial(pack_kernel, V, S, T, per),
        out_shape=jax.ShapeDtypeStruct((S * per + 1, R, LANES), f32),
        in_specs=[spec(SMEM), spec(VMEM), spec(pl.ANY)] + [spec(VMEM)] * 4,
        out_specs=spec(VMEM),
        scratch_shapes=[
            VMEM((T, SUB, G), f32),
            VMEM((nblk, LANES), i32),
            VMEM((SUB, nblk), i32),
            SMEM((SUB, nblk), i32),
            dma((T,)), dma,
        ],
        name="pack",
    )(meta, mask, attrs, means, scales, quats, peak)
    X = V // 2
    buf = pl.pallas_call(
        functools.partial(ship_kernel, V, S, per),
        out_shape=jax.ShapeDtypeStruct((V, S * per, R, LANES), f32),
        in_specs=[spec(VMEM)],
        out_specs=spec(pl.ANY),
        scratch_shapes=[
            dma((S,)), dma((X, S)), dma((X, S)), dma((2 * X, S)), dma,
        ],
        compiler_params=pltpu.CompilerParams(collective_id=1, has_side_effects=True),
        name="ship",
    )(packed)
    clones = pl.pallas_call(
        functools.partial(place_kernel, S, T, per),
        out_shape=jax.ShapeDtypeStruct((rows, G), f32),
        in_specs=[spec(SMEM), spec(VMEM)],
        out_specs=spec(VMEM),
        compiler_params=pltpu.CompilerParams(vmem_limit_bytes=32 * 1024 * 1024),
        name="place",
    )(meta, buf)
    return peak, clones, total


def solution(mesh):
    return jax.shard_map(
        functools.partial(body, mesh.shape["view"], mesh.shape["gauss"]),
        mesh=mesh,
        in_specs=(
            P(None, "gauss"),
            P(None, "gauss"),
            P(None, "gauss"),
            P(None, "gauss"),
            P("view", None, "gauss"),
            P("view", "gauss"),
            P("gauss"),
            P("view", None, None),
            P("view", None),
            P("view"),
        ),
        out_specs=(P(None, "gauss"), P(None, "gauss"), P()),
        check_vma=False,
    )
```

```python
import functools

import jax
import jax.numpy as jnp
from jax import lax
from jax.experimental import pallas as pl
from jax.experimental.pallas import tpu as pltpu
from jax.sharding import PartitionSpec as P

LANES = 128
SUB = 8
ATTR_TILES = 6
TILES = ATTR_TILES + 2
VMEM = pltpu.VMEM
SMEM = pltpu.SMEM
MESH = pl.DeviceIdType.MESH


def spec(space):
    return pl.BlockSpec(memory_space=space)


def peer(view, gauss):
    return {"view": view, "gauss": gauss}


def quat_factor(scales, quats):
    w, x, y, z = quats
    inv = 1.0 / jnp.sqrt(w * w + x * x + y * y + z * z + 0.25)
    w, x, y, z = (w * inv, x * inv, y * inv, z * inv)
    rq = [
        [1 - 2 * (y * y + z * z), 2 * (x * y - w * z), 2 * (x * z + w * y)],
        [2 * (x * y + w * z), 1 - 2 * (x * x + z * z), 2 * (y * z - w * x)],
        [2 * (x * z - w * y), 2 * (y * z + w * x), 1 - 2 * (x * x + y * y)],
    ]
    return [[rq[i][j] * scales[j] for j in range(3)] for i in range(3)]


def view_radius(means, factor, rot, trans, focal_v):
    point = [
        rot[i][0] * means[0] + rot[i][1] * means[1] + rot[i][2] * means[2] + trans[i]
        for i in range(3)
    ]
    inv = 1.0 / jnp.maximum(point[2], 1.0)
    j00 = focal_v * inv
    j02 = -(j00 * point[0]) * inv
    j12 = -(j00 * point[1]) * inv
    first = [j00 * rot[0][j] + j02 * rot[2][j] for j in range(3)]
    second = [j00 * rot[1][j] + j12 * rot[2][j] for j in range(3)]
    prow = [sum((first[j] * factor[j][k] for j in range(3))) for k in range(3)]
    qrow = [sum((second[j] * factor[j][k] for j in range(3))) for k in range(3)]
    a_val = prow[0] * prow[0] + prow[1] * prow[1] + prow[2] * prow[2] + 0.3
    c_val = qrow[0] * qrow[0] + qrow[1] * qrow[1] + qrow[2] * qrow[2] + 0.3
    b_val = prow[0] * qrow[0] + prow[1] * qrow[1] + prow[2] * qrow[2]
    half = 0.5 * (a_val - c_val)
    lam = 0.5 * (a_val + c_val) + jnp.sqrt(half * half + b_val * b_val + 0.01)
    return 3.0 * jnp.sqrt(lam)


def stats_kernel(
    V, S, views, rots, trns, foc, mask, means, scales, quats, grad, vis, peak, meta,
    cnt, counts, local, halves, merged, whole, total_max,
    csend, crecv, rsend, rrecv, gsend, grecv,
):
    v, s = lax.axis_index("view"), lax.axis_index("gauss")
    nblk = mask.shape[0]
    piece = 2 * nblk // V
    cnt[...] = jnp.full((SUB, LANES), jnp.sum(mask[...]), jnp.int32)
    bar = pltpu.get_barrier_semaphore()
    for k in range(1, S):
        pl.semaphore_signal(bar, inc=1, device_id=peer(v, lax.rem(s + k, S)), device_id_type=MESH)
    for k in range(1, V):
        pl.semaphore_signal(bar, inc=1, device_id=peer(lax.rem(v + k, V), s), device_id_type=MESH)

    step = 2 * SUB

    def chunk(i, carry):
        rows = pl.ds(pl.multiple_of(i * step, step), step)

        def lines(ref, count, c):
            return ref[pl.ds(i * step * count + c, step, stride=count), :]

        m = [means[rows, c, :] for c in range(3)]
        factor = quat_factor(
            [scales[rows, c, :] for c in range(3)], [lines(quats, 4, c) for c in range(4)]
        )
        gmax = jnp.zeros((step, LANES), jnp.float32)
        rmax = jnp.zeros((step, LANES), jnp.float32)
        for u in range(views):
            rot = [[rots[u, a, b] for b in range(3)] for a in range(3)]
            trans = [trns[u, a] for a in range(3)]
            radius = view_radius(m, factor, rot, trans, foc[u])
            seen = lines(vis, views, u).astype(jnp.float32)
            g0, g1 = (grad[u, pl.ds(i * step * 2 + c, step, stride=2), :] for c in range(2))
            gmax = jnp.maximum(gmax, jnp.sqrt(g0 * g0 + g1 * g1) * seen)
            rmax = jnp.maximum(rmax, radius * seen)
        local[pl.ds(i * step * 2, step, stride=2), :] = gmax
        local[pl.ds(i * step * 2 + 1, step, stride=2), :] = rmax
        return carry

    lax.fori_loop(0, nblk // step, chunk, 0)
    pl.semaphore_wait(bar, S + V - 2)
    copies = []
    for k in range(1, V):
        to = lax.rem(v + k, V)
        rs = pltpu.make_async_remote_copy(
            src_ref=local.at[pl.ds(pl.multiple_of(to * piece, piece), piece), :],
            dst_ref=halves.at[k],
            send_sem=rsend.at[k],
            recv_sem=rrecv.at[k],
            device_id=peer(to, s),
            device_id_type=MESH,
        )
        rs.start()
        copies.append(rs)
    tally = []
    for k in range(1, S):
        cp = pltpu.make_async_remote_copy(
            src_ref=cnt,
            dst_ref=counts.at[k],
            send_sem=csend.at[k],
            recv_sem=crecv.at[k],
            device_id=peer(v, lax.rem(s + k, S)),
            device_id_type=MESH,
        )
        cp.start()
        tally.append(cp)
    for rs in copies:
        rs.wait_recv()
    mine = pl.ds(pl.multiple_of(v * piece, piece), piece)
    best = local[mine, :]
    for k in range(1, V):
        best = jnp.maximum(best, halves[k])
    merged[...] = best
    spread = []
    for k in range(1, V):
        ag = pltpu.make_async_remote_copy(
            src_ref=merged,
            dst_ref=whole.at[k],
            send_sem=gsend.at[k],
            recv_sem=grecv.at[k],
            device_id=peer(lax.rem(v + k, V), s),
            device_id_type=MESH,
        )
        ag.start()
        spread.append(ag)
    for cp in tally:
        cp.wait_recv()
    lane = lax.broadcasted_iota(jnp.int32, (SUB, LANES), 1)
    sub = lax.broadcasted_iota(jnp.int32, (SUB, LANES), 0)
    blocks = jnp.zeros((SUB, LANES), jnp.int32)
    offs = jnp.zeros((SUB, LANES), jnp.int32)
    total = jnp.zeros((SUB, LANES), jnp.int32)
    for k in range(S):
        c = cnt[...] if k == 0 else counts[k]
        who = lax.rem(s + S - k, S)
        b = (c + (LANES - 1)) // LANES
        blocks = jnp.where(lane == who, b, blocks)
        offs = offs + jnp.where(lane > who, b, 0)
        total = total + c
    meta[...] = jnp.where(sub == 0, blocks, jnp.where(sub == 1, offs, total))
    total_max[mine, :] = best
    for k in range(1, V):
        spread[k - 1].wait_recv()
        who = lax.rem(v + V - k, V)
        total_max[pl.ds(pl.multiple_of(who * piece, piece), piece), :] = whole[k]
    for c in range(2):
        peak[:, c, :] = total_max[pl.ds(c, nblk, stride=2), :]
    for cp in copies + tally + spread:
        cp.wait_send()


def pack_kernel(
    V, S, T, per, meta, mask, attrs, means, scales, quats, peak, out,
    x, enc, basev, bases, sem, sem2,
):
    v, s = lax.axis_index("view"), lax.axis_index("gauss")
    nblk = mask.shape[0]
    for j in range(T):
        tile = v * T + j

        @pl.when(tile < ATTR_TILES)
        def _():
            pltpu.make_async_copy(
                attrs.at[pl.ds(pl.multiple_of(tile * SUB, SUB), SUB), :], x.at[j], sem.at[j]
            ).start()

        @pl.when(tile == ATTR_TILES + 1)
        def _():
            pltpu.make_async_copy(
                attrs.at[pl.ds(ATTR_TILES * SUB, 1), :], x.at[j, pl.ds(2, 1), :], sem.at[j]
            ).start()

    m = mask[...]
    lane = lax.broadcasted_iota(jnp.int32, (nblk, LANES), 1)
    mb = m.astype(jnp.bfloat16)
    li = lax.broadcasted_iota(jnp.int32, (LANES, LANES), 0)
    lj = lax.broadcasted_iota(jnp.int32, (LANES, LANES), 1)
    before = (li < lj).astype(jnp.bfloat16)
    bi = lax.broadcasted_iota(jnp.int32, (nblk, nblk), 0)
    bj = lax.broadcasted_iota(jnp.int32, (nblk, nblk), 1)
    above = (bi > bj).astype(jnp.bfloat16)
    under = (bi < bj).astype(jnp.bfloat16)
    dot = functools.partial(jnp.dot, preferred_element_type=jnp.float32)
    ones = jnp.ones((LANES, LANES), jnp.bfloat16)
    rank = dot(mb, before).astype(jnp.int32)
    size = dot(mb, ones).astype(jnp.int32)
    base = dot(dot(above, mb).astype(jnp.bfloat16), ones).astype(jnp.int32)
    flat = lax.dot_general(
        jnp.ones((SUB, LANES), jnp.bfloat16), mb, (((1,), (1,)), ((), ())),
        preferred_element_type=jnp.float32,
    )
    starts = dot(flat.astype(jnp.bfloat16), under)
    top = lax.broadcasted_iota(jnp.int32, (SUB, nblk), 0) == 0
    basev[...] = jnp.where(top, starts, starts + flat).astype(jnp.int32)
    scal = pltpu.make_async_copy(basev, bases, sem2)
    scal.start()
    code = jnp.where(m == 1, 65536 + (lane - rank) * 256 + lane, 0)
    bit = 1
    while bit < LANES:
        moved = pltpu.roll(code, LANES - bit, 1)
        goes = (moved & (bit * 256)) != 0
        stays = (code & (bit * 256)) == 0
        code = jnp.where(goes, moved, jnp.where(stays, code, 0))
        bit *= 2
    turn = (lane - base) & (LANES - 1)
    src = jnp.take_along_axis(code & (LANES - 1), turn, axis=1)
    enc[...] = jnp.where(turn < size, src, -1)

    for j in range(T):
        tile = v * T + j

        @pl.when(tile == ATTR_TILES)
        def _():
            x[j, 0:3, :] = means[...]
            x[j, 3:6, :] = scales[...]
            x[j, 6:8, :] = quats[0:2, :]

        @pl.when(tile == ATTR_TILES + 1)
        def _():
            x[j, 0:2, :] = quats[2:4, :]
            x[j, 3:5, :] = peak[...]
            x[j, 5:8, :] = jnp.zeros((3, peak.shape[1]), jnp.float32)
            pltpu.make_async_copy(
                attrs.at[pl.ds(ATTR_TILES * SUB, 1), :], x.at[j, pl.ds(2, 1), :], sem.at[j]
            ).wait()

        @pl.when(tile < ATTR_TILES)
        def _():
            pltpu.make_async_copy(attrs.at[pl.ds(0, SUB), :], x.at[j], sem.at[j]).wait()

    out[...] = jnp.zeros_like(out)
    scal.wait()
    offset = meta[1, s]
    row = lax.broadcasted_iota(jnp.int32, (SUB, LANES), 1)

    def spot(d):
        return jnp.where(d < nblk, lax.rem(offset + d, S) * per + lax.div(d, S), S * per)

    def move(b, cur):
        start = bases[0, b]
        off = lax.rem(start, LANES)
        d = lax.div(start, LANES)
        e = jnp.broadcast_to(enc[pl.ds(b, 1), :], (SUB, LANES))
        idx = jnp.maximum(e, 0)
        ok = e >= 0
        low = ok & (row >= off)
        high = ok & (row < off)
        where = spot(d)
        cols = pl.ds(pl.multiple_of(b * LANES, LANES), LANES)
        full = bases[1, b] >= (d + 1) * LANES
        nxt = []
        for j in range(T):
            g = jnp.take_along_axis(x[j, :, cols], idx, axis=1)
            keep = jnp.where(low, g, cur[j])
            out[where, j * SUB:(j + 1) * SUB, :] = keep
            nxt.append(jnp.where(full, jnp.where(high, g, 0.0), keep))
        return tuple(nxt)

    zero = jnp.zeros((SUB, LANES), jnp.float32)
    cur = lax.fori_loop(0, nblk, move, (zero,) * T, unroll=8)
    end = lax.div(bases[1, nblk - 1], LANES)
    for j in range(T):
        out[spot(end), j * SUB:(j + 1) * SUB, :] = cur[j]


def pair(s, k, S):
    if S & (S - 1):
        return lax.rem(s + k, S), lax.rem(s + S - k, S)
    t, bit = s, 1
    while bit < S:
        if k & bit:
            t = t + bit * (1 - 2 * lax.rem(lax.div(s, bit), 2))
        bit *= 2
    return t, t


def ship_kernel(V, S, per, src, buf, gsend, vsend, csend, recv, lsem):
    v, s = lax.axis_index("view"), lax.axis_index("gauss")
    core = lax.rem(v, 2)
    mate = v + 1 - 2 * core
    X = V // 2
    bar = pltpu.get_barrier_semaphore()
    for k in range(1, S):
        pl.semaphore_signal(bar, inc=1, device_id=peer(v, lax.rem(s + k, S)), device_id_type=MESH)
    for q in range(1, X):
        pl.semaphore_signal(
            bar, inc=1, device_id=peer(lax.rem(v + 2 * q, V), s), device_id_type=MESH
        )
    pl.semaphore_signal(bar, inc=1, device_id=peer(mate, s), device_id_type=MESH)
    pl.semaphore_wait(bar, S - 1 + X)

    def part(i):
        return pl.ds(i * per, per)

    def far(k):
        to = pair(s, k, S)[0]
        return pltpu.make_async_remote_copy(
            src_ref=src.at[part(to)], dst_ref=buf.at[v, part(s)],
            send_sem=gsend.at[k], recv_sem=recv.at[0, k],
            device_id=peer(v, to), device_id_type=MESH,
        )

    def at(k, q):
        owner = lax.rem(v + V - 2 * q, V)
        frm = pair(s, k, S)[1]
        if k == 0 and q == 0:
            return src.at[part(s)], owner, frm
        return buf.at[owner, part(frm)], owner, frm

    def across(k, q):
        ref, _, frm = at(k, 0)
        return pltpu.make_async_remote_copy(
            src_ref=ref, dst_ref=buf.at[v, part(frm)],
            send_sem=vsend.at[q, k], recv_sem=recv.at[q, k],
            device_id=peer(lax.rem(v + 2 * q, V), s), device_id_type=MESH,
        )

    def beside(k, q):
        ref, owner, frm = at(k, q)
        return pltpu.make_async_remote_copy(
            src_ref=ref, dst_ref=buf.at[owner, part(frm)],
            send_sem=csend.at[q, k], recv_sem=recv.at[X + q, k],
            device_id=peer(mate, s), device_id_type=MESH,
        )

    started = []

    def go(copy):
        copy.start()
        started.append(copy)

    fars = {k: far(k) for k in range(1, S)}
    for k in range(1, S):
        go(fars[k])
    for q in range(1, X):
        go(across(0, q))
    go(beside(0, 0))
    own = pltpu.make_async_copy(src.at[part(s)], buf.at[v, part(s)], lsem)
    own.start()
    for k in range(S):
        if k:
            fars[k].wait_recv()
            for q in range(1, X):
                go(across(k, q))
            go(beside(k, 0))
        if k:
            for q in range(1, X):
                across(k - 1, q).wait_recv()
                go(beside(k - 1, q))
    for q in range(1, X):
        across(S - 1, q).wait_recv()
        go(beside(S - 1, q))
    for k in range(S):
        for q in range(X):
            beside(k, q).wait_recv()
    for copy in started:
        copy.wait_send()
    own.wait()


def place_kernel(S, T, per, meta, buf, out):
    me = lax.axis_index("gauss")
    slots = out.shape[1] // LANES
    sub = lax.broadcasted_iota(jnp.int32, (SUB, LANES), 0)
    rows = out.shape[0]
    head = sub < 2
    filled = jnp.int32(0)
    for s in range(S):
        blocks, offset = meta[0, s], meta[1, s]
        first = lax.rem(me + S - lax.rem(offset, S), S)
        n = lax.div(jnp.maximum(blocks - first, 0) + (S - 1), S)
        slot0 = lax.div(offset + first, S)

        def one(w, carry):
            t = []
            for tile in range(TILES):
                j = tile % T
                t.append(buf[tile // T, s * per + w, j * SUB:(j + 1) * SUB, :])
            turned = [pltpu.roll(a, 2, 0) for a in t[:ATTR_TILES]]
            mixed = t[ATTR_TILES + 1]
            chain = [mixed] + turned + [mixed]
            cols = pl.ds(pl.multiple_of((slot0 + w) * LANES, LANES), LANES)
            out[0:SUB, cols] = t[ATTR_TILES]
            for i in range(1, TILES):
                value = jnp.where(head, chain[i - 1], chain[i])
                hi = min((i + 1) * SUB, rows)
                out[i * SUB:hi, cols] = value[: hi - i * SUB]
            return carry

        lax.fori_loop(0, n, one, 0)
        filled = filled + n

    def clear(q, carry):
        cols = pl.ds(pl.multiple_of(q * LANES, LANES), LANES)
        out[:, cols] = jnp.zeros((rows, LANES), jnp.float32)
        return carry

    lax.fori_loop(filled, slots, clear, 0)


def body(V, S, means, scales, quats, attrs, grad_screen, visible, clone_mask, rotation, shift, focal):
    G = clone_mask.shape[0]
    nblk = G // LANES
    views = grad_screen.shape[0]
    rows = means.shape[0] + scales.shape[0] + quats.shape[0] + attrs.shape[0] + 2
    T = -(-TILES // V)
    per = -(-nblk // S)
    f32, i32 = jnp.float32, jnp.int32
    mask = clone_mask.reshape(nblk, LANES)

    def lines(a):
        a = a.reshape(a.shape[:-1] + (nblk, LANES))
        return jnp.swapaxes(a, -3, -2)

    dma = pltpu.SemaphoreType.DMA
    piece = 2 * nblk // V
    peak2, meta = pl.pallas_call(
        functools.partial(stats_kernel, V, S, views),
        out_shape=(
            jax.ShapeDtypeStruct((nblk, 2, LANES), f32),
            jax.ShapeDtypeStruct((SUB, LANES), i32),
        ),
        in_specs=[spec(SMEM)] * 3 + [spec(VMEM)] * 6,
        out_specs=(spec(VMEM), spec(VMEM)),
        scratch_shapes=[
            VMEM((SUB, LANES), i32),
            VMEM((S, SUB, LANES), i32),
            VMEM((2 * nblk, LANES), f32),
            VMEM((V, piece, LANES), f32),
            VMEM((piece, LANES), f32),
            VMEM((V, piece, LANES), f32),
            VMEM((2 * nblk, LANES), f32),
            dma((S,)), dma((S,)), dma((V,)), dma((V,)), dma((V,)), dma((V,)),
        ],
        compiler_params=pltpu.CompilerParams(collective_id=0, has_side_effects=True),
        name="stats",
    )(
        rotation, shift, focal, mask, lines(means), lines(scales),
        lines(quats).reshape(-1, LANES), lines(grad_screen).reshape(views, -1, LANES),
        lines(visible).reshape(-1, LANES),
    )
    peak = jnp.swapaxes(peak2, 0, 1).reshape(2, G)
    total = meta[2, 0]
    R = T * SUB
    packed = pl.pallas_call(
        functools.partial(pack_kernel, V, S, T, per),
        out_shape=jax.ShapeDtypeStruct((S * per + 1, R, LANES), f32),
        in_specs=[spec(SMEM), spec(VMEM), spec(pl.ANY)] + [spec(VMEM)] * 4,
        out_specs=spec(VMEM),
        scratch_shapes=[
            VMEM((T, SUB, G), f32),
            VMEM((nblk, LANES), i32),
            VMEM((SUB, nblk), i32),
            SMEM((SUB, nblk), i32),
            dma((T,)), dma,
        ],
        name="pack",
    )(meta, mask, attrs, means, scales, quats, peak)
    X = V // 2
    buf = pl.pallas_call(
        functools.partial(ship_kernel, V, S, per),
        out_shape=jax.ShapeDtypeStruct((V, S * per, R, LANES), f32),
        in_specs=[spec(VMEM)],
        out_specs=spec(pl.ANY),
        scratch_shapes=[
            dma((S,)), dma((X, S)), dma((X, S)), dma((2 * X, S)), dma,
        ],
        compiler_params=pltpu.CompilerParams(collective_id=1, has_side_effects=True),
        name="ship",
    )(packed)
    clones = pl.pallas_call(
        functools.partial(place_kernel, S, T, per),
        out_shape=jax.ShapeDtypeStruct((rows, G), f32),
        in_specs=[spec(SMEM), spec(VMEM)],
        out_specs=spec(VMEM),
        compiler_params=pltpu.CompilerParams(vmem_limit_bytes=32 * 1024 * 1024),
        name="place",
    )(meta, buf)
    return peak, clones, total


def solution(mesh):
    return jax.shard_map(
        functools.partial(body, mesh.shape["view"], mesh.shape["gauss"]),
        mesh=mesh,
        in_specs=(
            P(None, "gauss"),
            P(None, "gauss"),
            P(None, "gauss"),
            P(None, "gauss"),
            P("view", None, "gauss"),
            P("view", "gauss"),
            P("gauss"),
            P("view", None, None),
            P("view", None),
            P("view"),
        ),
        out_specs=(P(None, "gauss"), P(None, "gauss"), P()),
        check_vma=False,
    )
```

```python
import functools

import jax
import jax.numpy as jnp
from jax import lax
from jax.experimental import pallas as pl
from jax.experimental.pallas import tpu as pltpu
from jax.sharding import PartitionSpec as P

LANES = 128
SUB = 8
ATTR_TILES = 6
TILES = ATTR_TILES + 2
VMEM = pltpu.VMEM
SMEM = pltpu.SMEM
MESH = pl.DeviceIdType.MESH


def spec(space):
    return pl.BlockSpec(memory_space=space)


def peer(view, gauss):
    return {"view": view, "gauss": gauss}


def quat_factor(scales, quats):
    w, x, y, z = quats
    inv = 1.0 / jnp.sqrt(w * w + x * x + y * y + z * z + 0.25)
    w, x, y, z = (w * inv, x * inv, y * inv, z * inv)
    rq = [
        [1 - 2 * (y * y + z * z), 2 * (x * y - w * z), 2 * (x * z + w * y)],
        [2 * (x * y + w * z), 1 - 2 * (x * x + z * z), 2 * (y * z - w * x)],
        [2 * (x * z - w * y), 2 * (y * z + w * x), 1 - 2 * (x * x + y * y)],
    ]
    return [[rq[i][j] * scales[j] for j in range(3)] for i in range(3)]


def view_radius(means, factor, rot, trans, focal_v):
    point = [
        rot[i][0] * means[0] + rot[i][1] * means[1] + rot[i][2] * means[2] + trans[i]
        for i in range(3)
    ]
    inv = 1.0 / jnp.maximum(point[2], 1.0)
    j00 = focal_v * inv
    j02 = -(j00 * point[0]) * inv
    j12 = -(j00 * point[1]) * inv
    first = [j00 * rot[0][j] + j02 * rot[2][j] for j in range(3)]
    second = [j00 * rot[1][j] + j12 * rot[2][j] for j in range(3)]
    prow = [sum((first[j] * factor[j][k] for j in range(3))) for k in range(3)]
    qrow = [sum((second[j] * factor[j][k] for j in range(3))) for k in range(3)]
    a_val = prow[0] * prow[0] + prow[1] * prow[1] + prow[2] * prow[2] + 0.3
    c_val = qrow[0] * qrow[0] + qrow[1] * qrow[1] + qrow[2] * qrow[2] + 0.3
    b_val = prow[0] * qrow[0] + prow[1] * qrow[1] + prow[2] * qrow[2]
    half = 0.5 * (a_val - c_val)
    lam = 0.5 * (a_val + c_val) + jnp.sqrt(half * half + b_val * b_val + 0.01)
    return 3.0 * jnp.sqrt(lam)


def stats_kernel(
    S, views, rots, trns, foc, mask, means, scales, quats, grad, vis, local, meta,
    cnt, counts, csend, crecv,
):
    v, s = lax.axis_index("view"), lax.axis_index("gauss")
    nblk = mask.shape[0]
    cnt[...] = jnp.full((SUB, LANES), jnp.sum(mask[...]), jnp.int32)
    bar = pltpu.get_barrier_semaphore()
    for k in range(1, S):
        pl.semaphore_signal(bar, inc=1, device_id=peer(v, lax.rem(s + k, S)), device_id_type=MESH)
    pl.semaphore_wait(bar, S - 1)
    tally = []
    for k in range(1, S):
        cp = pltpu.make_async_remote_copy(
            src_ref=cnt,
            dst_ref=counts.at[k],
            send_sem=csend.at[k],
            recv_sem=crecv.at[k],
            device_id=peer(v, lax.rem(s + k, S)),
            device_id_type=MESH,
        )
        cp.start()
        tally.append(cp)

    step = 2 * SUB

    def chunk(i, carry):
        rows = pl.ds(pl.multiple_of(i * step, step), step)

        def lines(ref, count, c):
            return ref[pl.ds(i * step * count + c, step, stride=count), :]

        m = [means[rows, c, :] for c in range(3)]
        factor = quat_factor(
            [scales[rows, c, :] for c in range(3)], [lines(quats, 4, c) for c in range(4)]
        )
        gmax = jnp.zeros((step, LANES), jnp.float32)
        rmax = jnp.zeros((step, LANES), jnp.float32)
        for u in range(views):
            rot = [[rots[u, a, b] for b in range(3)] for a in range(3)]
            trans = [trns[u, a] for a in range(3)]
            radius = view_radius(m, factor, rot, trans, foc[u])
            seen = lines(vis, views, u).astype(jnp.float32)
            g0, g1 = (grad[u, pl.ds(i * step * 2 + c, step, stride=2), :] for c in range(2))
            gmax = jnp.maximum(gmax, jnp.sqrt(g0 * g0 + g1 * g1) * seen)
            rmax = jnp.maximum(rmax, radius * seen)
        local[pl.ds(i * step * 2, step, stride=2), :] = gmax
        local[pl.ds(i * step * 2 + 1, step, stride=2), :] = rmax
        return carry

    lax.fori_loop(0, nblk // step, chunk, 0)
    for cp in tally:
        cp.wait_recv()
    lane = lax.broadcasted_iota(jnp.int32, (SUB, LANES), 1)
    sub = lax.broadcasted_iota(jnp.int32, (SUB, LANES), 0)
    blocks = jnp.zeros((SUB, LANES), jnp.int32)
    offs = jnp.zeros((SUB, LANES), jnp.int32)
    total = jnp.zeros((SUB, LANES), jnp.int32)
    for k in range(S):
        c = cnt[...] if k == 0 else counts[k]
        who = lax.rem(s + S - k, S)
        b = (c + (LANES - 1)) // LANES
        blocks = jnp.where(lane == who, b, blocks)
        offs = offs + jnp.where(lane > who, b, 0)
        total = total + c
    meta[...] = jnp.where(sub == 0, blocks, jnp.where(sub == 1, offs, total))
    for cp in tally:
        cp.wait_send()


def pack_kernel(
    V, S, T, per, meta, mask, attrs, means, scales, quats, out, order,
    x, enc, basev, bases, sem, sem2,
):
    v, s = lax.axis_index("view"), lax.axis_index("gauss")
    nblk = mask.shape[0]
    for j in range(T):
        tile = v * T + j

        @pl.when(tile < ATTR_TILES)
        def _():
            pltpu.make_async_copy(
                attrs.at[pl.ds(pl.multiple_of(tile * SUB, SUB), SUB), :], x.at[j], sem.at[j]
            ).start()

        @pl.when(tile == ATTR_TILES + 1)
        def _():
            pltpu.make_async_copy(
                attrs.at[pl.ds(ATTR_TILES * SUB, 1), :], x.at[j, pl.ds(2, 1), :], sem.at[j]
            ).start()

    m = mask[...]
    lane = lax.broadcasted_iota(jnp.int32, (nblk, LANES), 1)
    mb = m.astype(jnp.bfloat16)
    li = lax.broadcasted_iota(jnp.int32, (LANES, LANES), 0)
    lj = lax.broadcasted_iota(jnp.int32, (LANES, LANES), 1)
    before = (li < lj).astype(jnp.bfloat16)
    bi = lax.broadcasted_iota(jnp.int32, (nblk, nblk), 0)
    bj = lax.broadcasted_iota(jnp.int32, (nblk, nblk), 1)
    above = (bi > bj).astype(jnp.bfloat16)
    under = (bi < bj).astype(jnp.bfloat16)
    dot = functools.partial(jnp.dot, preferred_element_type=jnp.float32)
    ones = jnp.ones((LANES, LANES), jnp.bfloat16)
    rank = dot(mb, before).astype(jnp.int32)
    size = dot(mb, ones).astype(jnp.int32)
    base = dot(dot(above, mb).astype(jnp.bfloat16), ones).astype(jnp.int32)
    flat = lax.dot_general(
        jnp.ones((SUB, LANES), jnp.bfloat16), mb, (((1,), (1,)), ((), ())),
        preferred_element_type=jnp.float32,
    )
    starts = dot(flat.astype(jnp.bfloat16), under)
    top = lax.broadcasted_iota(jnp.int32, (SUB, nblk), 0) == 0
    basev[...] = jnp.where(top, starts, starts + flat).astype(jnp.int32)
    scal = pltpu.make_async_copy(basev, bases, sem2)
    scal.start()
    code = jnp.where(m == 1, 65536 + (lane - rank) * 256 + lane, 0)
    bit = 1
    while bit < LANES:
        moved = pltpu.roll(code, LANES - bit, 1)
        goes = (moved & (bit * 256)) != 0
        stays = (code & (bit * 256)) == 0
        code = jnp.where(goes, moved, jnp.where(stays, code, 0))
        bit *= 2
    turn = (lane - base) & (LANES - 1)
    src = jnp.take_along_axis(code & (LANES - 1), turn, axis=1)
    enc[...] = jnp.where(turn < size, src, -1)

    for j in range(T):
        tile = v * T + j

        @pl.when(tile == ATTR_TILES)
        def _():
            x[j, 0:3, :] = means[...]
            x[j, 3:6, :] = scales[...]
            x[j, 6:8, :] = quats[0:2, :]

        @pl.when(tile == ATTR_TILES + 1)
        def _():
            x[j, 0:2, :] = quats[2:4, :]
            x[j, 3:8, :] = jnp.zeros((5, quats.shape[1]), jnp.float32)
            pltpu.make_async_copy(
                attrs.at[pl.ds(ATTR_TILES * SUB, 1), :], x.at[j, pl.ds(2, 1), :], sem.at[j]
            ).wait()

        @pl.when(tile < ATTR_TILES)
        def _():
            pltpu.make_async_copy(attrs.at[pl.ds(0, SUB), :], x.at[j], sem.at[j]).wait()

    out[...] = jnp.zeros_like(out)
    order[...] = jnp.full_like(order, -1)
    scal.wait()
    offset = meta[1, s]
    row = lax.broadcasted_iota(jnp.int32, (SUB, LANES), 1)

    def spot(d):
        return jnp.where(d < nblk, lax.rem(offset + d, S) * per + lax.div(d, S), S * per)

    def move(b, cur):
        start = bases[0, b]
        off = lax.rem(start, LANES)
        d = lax.div(start, LANES)
        e = jnp.broadcast_to(enc[pl.ds(b, 1), :], (SUB, LANES))
        idx = jnp.maximum(e, 0)
        ok = e >= 0
        low = ok & (row >= off)
        high = ok & (row < off)
        where = spot(d)
        cols = pl.ds(pl.multiple_of(b * LANES, LANES), LANES)
        full = bases[1, b] >= (d + 1) * LANES
        gid = b * LANES + idx
        keep = jnp.where(low, gid, cur[T])
        order[pl.ds(where, 1), :] = keep[0:1]
        last = jnp.where(full, jnp.where(high, gid, -1), keep)
        nxt = []
        for j in range(T):
            g = jnp.take_along_axis(x[j, :, cols], idx, axis=1)
            keep = jnp.where(low, g, cur[j])
            out[where, j * SUB:(j + 1) * SUB, :] = keep
            nxt.append(jnp.where(full, jnp.where(high, g, 0.0), keep))
        return tuple(nxt) + (last,)

    zero = jnp.zeros((SUB, LANES), jnp.float32)
    cur = lax.fori_loop(0, nblk, move, (zero,) * T + (jnp.full((SUB, LANES), -1, jnp.int32),), unroll=8)
    end = lax.div(bases[1, nblk - 1], LANES)
    for j in range(T):
        out[spot(end), j * SUB:(j + 1) * SUB, :] = cur[j]
    order[pl.ds(spot(end), 1), :] = cur[T][0:1]


def pair(s, k, S):
    if S & (S - 1):
        return lax.rem(s + k, S), lax.rem(s + S - k, S)
    t, bit = s, 1
    while bit < S:
        if k & bit:
            t = t + bit * (1 - 2 * lax.rem(lax.div(s, bit), 2))
        bit *= 2
    return t, t


def ship_kernel(
    V, S, T, per, src, local, order, buf, peak,
    halves, merged, whole, best, tile,
    rsend, rrecv, msend, mrecv, gsend, vsend, csend, recv, lsem,
):
    v, s = lax.axis_index("view"), lax.axis_index("gauss")
    core = lax.rem(v, 2)
    mate = v + 1 - 2 * core
    X = V // 2
    nblk = peak.shape[0]
    piece = 2 * nblk // V
    bar = pltpu.get_barrier_semaphore()
    for k in range(1, S):
        pl.semaphore_signal(bar, inc=1, device_id=peer(v, lax.rem(s + k, S)), device_id_type=MESH)
    for k in range(1, V):
        pl.semaphore_signal(bar, inc=1, device_id=peer(lax.rem(v + k, V), s), device_id_type=MESH)
    pl.semaphore_wait(bar, S + V - 2)
    started = []

    def go(copy):
        copy.start()
        started.append(copy)

    def part(i):
        return pl.ds(i * per, per)

    def row(j):
        return pl.ds(j * SUB, SUB)

    def mine(i, j):
        return tile.at[part(i)] if j == T - 1 else src.at[part(i), row(j), :]

    def remote(ref, owner, frm, j, send, sem, to):
        return pltpu.make_async_remote_copy(
            src_ref=ref, dst_ref=buf.at[owner, part(frm), row(j), :],
            send_sem=send, recv_sem=sem, device_id=to, device_id_type=MESH,
        )

    def far(k, j):
        to = pair(s, k, S)[0]
        return remote(mine(to, j), v, s, j, gsend.at[k, j], recv.at[0, k, j], peer(v, to))

    def at(k, q, j):
        owner = lax.rem(v + V - 2 * q, V)
        frm = pair(s, k, S)[1]
        if k == 0 and q == 0:
            return mine(s, j), owner, frm
        return buf.at[owner, part(frm), row(j), :], owner, frm

    def across(k, q, j):
        ref, _, frm = at(k, 0, j)
        to = peer(lax.rem(v + 2 * q, V), s)
        return remote(ref, v, frm, j, vsend.at[q, k, j], recv.at[q, k, j], to)

    def beside(k, q, j):
        ref, owner, frm = at(k, q, j)
        return remote(
            ref, owner, frm, j, csend.at[q, k, j], recv.at[X + q, k, j], peer(mate, s)
        )

    def forward(k, j):
        if k:
            far(k, j).wait_recv()
        for q in range(1, X):
            go(across(k, q, j))
        go(beside(k, 0, j))

    def relay(k, j):
        for q in range(1, X):
            across(k, q, j).wait_recv()
            go(beside(k, q, j))

    def lot(i):
        return pl.ds(pl.multiple_of(i * piece, piece), piece)

    halve = []
    for k in range(1, V):
        to = lax.rem(v + k, V)
        halve.append(pltpu.make_async_remote_copy(
            src_ref=local.at[lot(to), :], dst_ref=halves.at[k],
            send_sem=rsend.at[k], recv_sem=rrecv.at[k],
            device_id=peer(to, s), device_id_type=MESH,
        ))
        go(halve[-1])
    for j in range(T - 1):
        for k in range(1, S):
            go(far(k, j))
        forward(0, j)
    tile[...] = src[0:S * per, (T - 1) * SUB:T * SUB, :]
    for copy in halve:
        copy.wait_recv()
    top = local[lot(v), :]
    for k in range(1, V):
        top = jnp.maximum(top, halves[k])
    merged[...] = top
    best[lot(v), :] = top
    spread = []
    for k in range(1, V):
        spread.append(pltpu.make_async_remote_copy(
            src_ref=merged, dst_ref=whole.at[k],
            send_sem=msend.at[k], recv_sem=mrecv.at[k],
            device_id=peer(lax.rem(v + k, V), s), device_id_type=MESH,
        ))
        go(spread[-1])
    for j in range(T - 1):
        forward(1, j)
    for k in range(1, V):
        spread[k - 1].wait_recv()
        best[lot(lax.rem(v + V - k, V)), :] = whole[k]
    for c in range(2):
        peak[:, c, :] = best[pl.ds(c, nblk, stride=2), :]

    @pl.when(v * T + T == TILES)
    def _():
        group = 4 * SUB

        def fetch(i, carry):
            rows = pl.ds(pl.multiple_of(i * group, group), group)
            idx = order[rows, :]
            blk, lane = idx >> 7, idx & (LANES - 1)

            def look(b, acc):
                hit = blk == b
                return tuple(
                    jnp.where(
                        hit,
                        jnp.take_along_axis(
                            jnp.broadcast_to(best[pl.ds(2 * b + c, 1), :], idx.shape), lane, axis=1
                        ),
                        acc[c],
                    )
                    for c in range(2)
                )

            zero = jnp.zeros(idx.shape, jnp.float32)
            acc = lax.fori_loop(0, nblk, look, (zero, zero), unroll=4)
            tile[rows, 3, :] = acc[0]
            tile[rows, 4, :] = acc[1]
            return carry

        lax.fori_loop(0, S * per // group, fetch, 0)

    for k in range(1, S):
        go(far(k, T - 1))
    own = []
    for j in range(T):
        own.append(pltpu.make_async_copy(mine(s, j), buf.at[v, part(s), row(j), :], lsem.at[j]))
        own[-1].start()
    for j in range(T - 1):
        relay(0, j)
        for k in range(2, S):
            forward(k, j)
            relay(k - 1, j)
            if k == 2:
                forward(0, T - 1)
        relay(S - 1, j)
    if T == 1:
        forward(0, T - 1)
    for k in range(1, S):
        forward(k, T - 1)
        relay(k - 1, T - 1)
    relay(S - 1, T - 1)
    for j in range(T):
        for k in range(S):
            for q in range(X):
                beside(k, q, j).wait_recv()
    for copy in started:
        copy.wait_send()
    for copy in own:
        copy.wait()


def place_kernel(S, T, per, meta, buf, out):
    me = lax.axis_index("gauss")
    slots = out.shape[1] // LANES
    sub = lax.broadcasted_iota(jnp.int32, (SUB, LANES), 0)
    rows = out.shape[0]
    head = sub < 2
    filled = jnp.int32(0)
    for s in range(S):
        blocks, offset = meta[0, s], meta[1, s]
        first = lax.rem(me + S - lax.rem(offset, S), S)
        n = lax.div(jnp.maximum(blocks - first, 0) + (S - 1), S)
        slot0 = lax.div(offset + first, S)

        def one(w, carry):
            t = []
            for tile in range(TILES):
                j = tile % T
                t.append(buf[tile // T, s * per + w, j * SUB:(j + 1) * SUB, :])
            turned = [pltpu.roll(a, 2, 0) for a in t[:ATTR_TILES]]
            mixed = t[ATTR_TILES + 1]
            chain = [mixed] + turned + [mixed]
            cols = pl.ds(pl.multiple_of((slot0 + w) * LANES, LANES), LANES)
            out[0:SUB, cols] = t[ATTR_TILES]
            for i in range(1, TILES):
                value = jnp.where(head, chain[i - 1], chain[i])
                hi = min((i + 1) * SUB, rows)
                out[i * SUB:hi, cols] = value[: hi - i * SUB]
            return carry

        lax.fori_loop(0, n, one, 0)
        filled = filled + n

    def clear(q, carry):
        cols = pl.ds(pl.multiple_of(q * LANES, LANES), LANES)
        out[:, cols] = jnp.zeros((rows, LANES), jnp.float32)
        return carry

    lax.fori_loop(filled, slots, clear, 0)


def body(V, S, means, scales, quats, attrs, grad_screen, visible, clone_mask, rotation, shift, focal):
    G = clone_mask.shape[0]
    nblk = G // LANES
    views = grad_screen.shape[0]
    rows = means.shape[0] + scales.shape[0] + quats.shape[0] + attrs.shape[0] + 2
    T = -(-TILES // V)
    per = -(-nblk // S)
    f32, i32 = jnp.float32, jnp.int32
    mask = clone_mask.reshape(nblk, LANES)

    def lines(a):
        a = a.reshape(a.shape[:-1] + (nblk, LANES))
        return jnp.swapaxes(a, -3, -2)

    dma = pltpu.SemaphoreType.DMA
    piece = 2 * nblk // V
    local, meta = pl.pallas_call(
        functools.partial(stats_kernel, S, views),
        out_shape=(
            jax.ShapeDtypeStruct((2 * nblk, LANES), f32),
            jax.ShapeDtypeStruct((SUB, LANES), i32),
        ),
        in_specs=[spec(SMEM)] * 3 + [spec(VMEM)] * 6,
        out_specs=(spec(VMEM), spec(VMEM)),
        scratch_shapes=[
            VMEM((SUB, LANES), i32), VMEM((S, SUB, LANES), i32), dma((S,)), dma((S,)),
        ],
        compiler_params=pltpu.CompilerParams(collective_id=0, has_side_effects=True),
        name="stats",
    )(
        rotation, shift, focal, mask, lines(means), lines(scales),
        lines(quats).reshape(-1, LANES), lines(grad_screen).reshape(views, -1, LANES),
        lines(visible).reshape(-1, LANES),
    )
    total = meta[2, 0]
    R = T * SUB
    X = V // 2
    packed, order = pl.pallas_call(
        functools.partial(pack_kernel, V, S, T, per),
        out_shape=(
            jax.ShapeDtypeStruct((S * per + 1, R, LANES), f32),
            jax.ShapeDtypeStruct((S * per + SUB, LANES), i32),
        ),
        in_specs=[spec(SMEM), spec(VMEM), spec(pl.ANY)] + [spec(VMEM)] * 3,
        out_specs=(spec(VMEM), spec(VMEM)),
        scratch_shapes=[
            VMEM((T, SUB, G), f32),
            VMEM((nblk, LANES), i32),
            VMEM((SUB, nblk), i32),
            SMEM((SUB, nblk), i32),
            dma((T,)), dma,
        ],
        name="pack",
    )(meta, mask, attrs, means, scales, quats)
    buf, peak2 = pl.pallas_call(
        functools.partial(ship_kernel, V, S, T, per),
        out_shape=(
            jax.ShapeDtypeStruct((V, S * per, R, LANES), f32),
            jax.ShapeDtypeStruct((nblk, 2, LANES), f32),
        ),
        in_specs=[spec(VMEM)] * 3,
        out_specs=(spec(pl.ANY), spec(VMEM)),
        scratch_shapes=[
            VMEM((V, piece, LANES), f32),
            VMEM((piece, LANES), f32),
            VMEM((V, piece, LANES), f32),
            VMEM((2 * nblk, LANES), f32),
            VMEM((S * per, SUB, LANES), f32),
            dma((V,)), dma((V,)), dma((V,)), dma((V,)),
            dma((S, T)), dma((X, S, T)), dma((X, S, T)), dma((2 * X, S, T)), dma((T,)),
        ],
        compiler_params=pltpu.CompilerParams(collective_id=1, has_side_effects=True),
        name="ship",
    )(packed, local, order)
    peak = jnp.swapaxes(peak2, 0, 1).reshape(2, G)
    clones = pl.pallas_call(
        functools.partial(place_kernel, S, T, per),
        out_shape=jax.ShapeDtypeStruct((rows, G), f32),
        in_specs=[spec(SMEM), spec(VMEM)],
        out_specs=spec(VMEM),
        compiler_params=pltpu.CompilerParams(vmem_limit_bytes=32 * 1024 * 1024),
        name="place",
    )(meta, buf)
    return peak, clones, total


def solution(mesh):
    return jax.shard_map(
        functools.partial(body, mesh.shape["view"], mesh.shape["gauss"]),
        mesh=mesh,
        in_specs=(
            P(None, "gauss"),
            P(None, "gauss"),
            P(None, "gauss"),
            P(None, "gauss"),
            P("view", None, "gauss"),
            P("view", "gauss"),
            P("gauss"),
            P("view", None, None),
            P("view", None),
            P("view"),
        ),
        out_specs=(P(None, "gauss"), P(None, "gauss"), P()),
        check_vma=False,
    )
```
